32 devices in a mesh: req: 2 (over y), patch: 16 (over z, x, core).
Axes of the slice: x: 2, y: 2, z: 4, core: 2. Of those that a mesh axis runs over, the one named last changes fastest.
Arguments:
- tokens: bfloat16 [1536, 1152], P(('req', 'patch')), parts along dimension 0, may hold values from -6 to 6
- positions: int32 [2, 1536], P(None, ('req', 'patch')), parts along dimension 1, may hold values from 0 to 95
- counts: int32 [32], P('req'), parts along dimension 0, may hold values from 1 to 48, 384 in all
- timestep: int32 [2], P('req'), parts along dimension 0, may hold values from 0 to 999
- time_in: bfloat16 [256, 1152], replicated, may hold values from -0.375 to 0.375
- time_out: bfloat16 [1152, 1152], P(None, 'patch'), may hold values from -0.1875 to 0.1875
- ada_weight: bfloat16 [1152, 3456], P('patch'), may hold values from -0.375 to 0.375
- qkv_weight: bfloat16 [1152, 3456], replicated, may hold values from -2 to 2, as said below
- out_weight: bfloat16 [1152, 1152], replicated, may hold values from -0.1875 to 0.1875
Outputs:
- block_out: bfloat16 [1536, 1152], P(('req', 'patch')), parts along dimension 0
The draws below stay inside these ranges and needn't reach their ends.
There are 2 independent parts, one for each index of `req`. The reference program is written for one: setup_inputs(seed, part) draws one part's arguments, and reference() takes and returns one part's arrays. A program takes and returns all parts, laid end to end along the dimension named above; an argument that names none is the same for every part. Nothing has to cross between parts.
Inputs may be any that keep to these rules, and one draw needn't show every extreme that they name: `counts`: used slots are the first ones of each block; they sum to exactly 384, and some block uses all 48. `qkv_weight`: columns are 1152 of queries, 1152 of keys, 1152 of values, each head's 72 columns side by side.
All inputs are finite; a program needn't handle non-finite values.
Results may differ from the reference program's by a relative error of at most 0.0039.
Values may be sent and summed in bfloat16 or wider, within the bound.
A program may use at most 64 MiB of HBM per device.

```python
import math
import jax
import jax.numpy as jnp
import numpy as np
from jax import lax

D = 1152
HEADS = 16
HEAD_DIM = 72
FREQ = 256
TOK_DEV = 48
SLOTS = 768
VALID = 384
N_PATCH = 16


def draw_qkv_weight(key, part):
    base_values = jax.random.truncated_normal(key, -4.0, 4.0, (D, 3 * D), jnp.float32) / math.sqrt(D)
    column_kind = jnp.arange(3 * D) // D
    scaled = base_values * jnp.where(column_kind < 2, 1.3, 1.0)[None, :]
    return jnp.clip(scaled, -2.0, 2.0).astype(jnp.bfloat16)


def set_ends(values, stream_key, low, high):
    place = [jax.random.randint(jax.random.fold_in(stream_key, axis), (), 0, length) for axis, length in enumerate(values.shape)]
    widest = values.shape.index(max(values.shape))
    neighbour = place[:widest] + [(place[widest] + 1) % values.shape[widest]] + place[widest + 1:]
    return values.at[tuple(place)].set(low).at[tuple(neighbour)].set(high)


def level_of(key, shape, split, smallest, top_value):
    def one(position, blocks):
        draws = jax.random.uniform(jax.random.fold_in(jax.random.fold_in(key, 6), position), (blocks,), jnp.float32, smallest / len(split), top_value / len(split))
        return jnp.repeat(jnp.exp(draws), shape[position] // blocks).reshape((-1,) + (1,) * (len(shape) - position - 1))

    gain = one(*split[0])
    for cut in split[1:]:
        gain = gain * one(*cut)
    return gain


def length_profile(number_of, total, reach, skew):
    portions = [(1 << 20) // math.isqrt(standing ** skew) + 1 for standing in range(2, number_of + 1)]
    spare, holding = total - reach - (number_of - 1), [1] * (number_of - 1)
    while spare > 0:
        movable = [i for i in range(number_of - 1) if holding[i] < reach]
        mass, budget = sum([portions[i] for i in movable]), spare
        for i in movable:
            extra = min(reach - holding[i], max(1, budget * portions[i] // mass), spare)
            holding[i] = holding[i] + extra
            spare = spare - extra
    return np.array([reach] + holding)


def uneven_parts(key, count, total, most, skew):
    if count == 2:
        one = jax.random.randint(key, (), max(1, total - most), min(most, total - 1) + 1)
        return jnp.stack([one, total - one])
    tallies = jnp.asarray(length_profile(count, total, most, skew), jnp.int32)
    pairs = (count - 1) // 2
    donor, sink = tallies[1:1 + 2 * pairs:2], tallies[2:2 + 2 * pairs:2]
    room = jnp.minimum(donor - 1, most - sink)
    moved = jax.random.randint(jax.random.fold_in(key, 1), (pairs,), 0, 1 << 20) % (room + 1)
    tallies = tallies.at[1:1 + 2 * pairs:2].set(donor - moved).at[2:2 + 2 * pairs:2].set(sink + moved)
    return tallies[jax.random.permutation(jax.random.fold_in(key, 2), count)]


def noise(key, shape, deviation, reach, pieces=(), kind=jnp.bfloat16):
    loudness = level_of(key, shape, pieces, -0.22, 0.18) if pieces else 1.0
    drawn = jax.random.normal(key, shape, jnp.float32) * deviation * loudness
    return jnp.minimum(jnp.maximum(drawn, -reach), reach).astype(kind)


def setup_inputs(seed: int = 0, part: int = 0) -> dict:
    streams_of = jax.random.split(jax.random.key(seed), 10)
    own_keys = jax.random.split(jax.random.fold_in(streams_of[9], part), 10)
    tokens = noise(own_keys[0], (SLOTS, D), 1.0, 6.0, ((0, 16),))
    positions = set_ends(jax.random.randint(own_keys[1], (2, SLOTS), 0, 96), jax.random.fold_in(own_keys[1], 1), 0, 95).astype(jnp.int32)
    counts = uneven_parts(own_keys[2], N_PATCH, VALID, TOK_DEV, 2).astype(jnp.int32)
    timestep = jax.random.randint(own_keys[3], (1,), 0, 1000).astype(jnp.int32)
    time_in = noise(streams_of[4], (FREQ, D), FREQ ** -0.5, 0.375)
    time_out = noise(streams_of[5], (D, D), D ** -0.5, 0.1875, ((1, 16),))
    ada_weight = noise(streams_of[6], (D, 3 * D), (D // 4) ** -0.5, 0.375, ((0, 16),))
    qkv_weight = draw_qkv_weight(jax.random.fold_in(streams_of[9], 71), part)
    out_weight = noise(streams_of[8], (D, D), D ** -0.5, 0.1875)
    return dict(tokens=tokens, positions=positions, counts=counts, timestep=timestep, time_in=time_in, time_out=time_out, ada_weight=ada_weight, qkv_weight=qkv_weight, out_weight=out_weight)


def time_features(timestep, freq_size):
    half_size = freq_size // 2
    frequencies = jnp.exp(-math.log(10000.0) * jnp.arange(half_size, dtype=jnp.float32) / half_size)
    angles = timestep.astype(jnp.float32)[:, None] * frequencies[None, :]
    return jnp.concatenate([jnp.cos(angles), jnp.sin(angles)], axis=1).astype(jnp.bfloat16)

def position_table(positions, model_width):
    quarter = model_width // 4
    omegas = jnp.power(10000.0, -jnp.arange(quarter, dtype=jnp.float32) / quarter)
    row_angle = positions[0].astype(jnp.float32)[:, None] * omegas[None, :]
    col_angle = positions[1].astype(jnp.float32)[:, None] * omegas[None, :]
    return jnp.concatenate([jnp.sin(row_angle), jnp.cos(row_angle), jnp.sin(col_angle), jnp.cos(col_angle)], axis=1)

def reference(tokens, positions, counts, timestep, time_in, time_out, ada_weight, qkv_weight, out_weight):
    model_width = tokens.shape[1]
    slot_count = tokens.shape[0]
    per_device = slot_count // N_PATCH
    features = time_features(timestep, FREQ)
    hidden_time = jax.nn.silu(jnp.dot(features, time_in, preferred_element_type=jnp.float32)).astype(jnp.bfloat16)
    cond = jnp.dot(hidden_time, time_out, preferred_element_type=jnp.float32)
    activated = jax.nn.silu(cond).astype(jnp.bfloat16)
    modulation = jnp.dot(activated, ada_weight, preferred_element_type=jnp.float32)
    shift_mod = modulation[:, :model_width]
    scale_mod = modulation[:, model_width:2 * model_width]
    gate_mod = modulation[:, 2 * model_width:]
    x_in = tokens.astype(jnp.float32) + position_table(positions, model_width)
    mean_value = lax.optimization_barrier(jnp.mean(x_in, axis=1, keepdims=True))
    centered = x_in - mean_value
    variance = lax.optimization_barrier(jnp.mean(centered * centered, axis=1, keepdims=True))
    normed = centered * lax.rsqrt(variance + 1e-06)
    modulated = (normed * (1.0 + scale_mod) + shift_mod).astype(jnp.bfloat16)
    projections = jnp.dot(modulated, qkv_weight, preferred_element_type=jnp.float32).astype(jnp.bfloat16)
    slot_valid = (jnp.arange(per_device, dtype=jnp.int32)[None, :] < counts[:, None]).reshape(slot_count)
    key_heads = projections[:, model_width:2 * model_width].astype(jnp.float32).reshape(slot_count, HEADS, HEAD_DIM)
    value_heads = projections[:, 2 * model_width:].astype(jnp.float32).reshape(slot_count, HEADS, HEAD_DIM)
    query_blocks = projections[:, :model_width].astype(jnp.float32).reshape(N_PATCH, per_device, HEADS, HEAD_DIM)
    inv_root = 1.0 / math.sqrt(HEAD_DIM)

    def attend(query_block):
        scores = jnp.einsum('qhd,khd->hqk', query_block, key_heads, precision=lax.Precision.HIGHEST) * inv_root
        scores = jnp.where(slot_valid[None, None, :], scores, -1e+30)
        row_top = lax.optimization_barrier(jnp.max(scores, axis=2, keepdims=True))
        weights = jnp.where(slot_valid[None, None, :], jnp.exp(scores - row_top), 0.0)
        denominator = lax.optimization_barrier(jnp.sum(weights, axis=2, keepdims=True))
        rounded = lax.optimization_barrier(weights.astype(jnp.bfloat16))
        weighted = jnp.einsum('hqk,khd->qhd', rounded.astype(jnp.float32), value_heads, precision=lax.Precision.HIGHEST)
        return weighted / jnp.transpose(denominator, (1, 0, 2))
    attended = lax.map(attend, query_blocks).reshape(slot_count, model_width).astype(jnp.bfloat16)
    projected = jnp.dot(attended, out_weight, preferred_element_type=jnp.float32)
    valid_column = slot_valid.astype(jnp.float32)[:, None]
    return (x_in + gate_mod * projected * valid_column).astype(jnp.bfloat16)
```

```python
import math

import jax
import jax.numpy as jnp
from jax import lax
from jax.sharding import PartitionSpec as P

HEADS = 16


neg_large = -1e30
key_block = 512


def time_features(timestep, freq_size):
    half_size = freq_size // 2
    frequencies = jnp.exp(-math.log(10000.0) * jnp.arange(half_size, dtype=jnp.float32) / half_size)
    angles = timestep.astype(jnp.float32)[:, None] * frequencies[None, :]
    return jnp.concatenate([jnp.cos(angles), jnp.sin(angles)], axis=1).astype(jnp.bfloat16)


def position_table(positions, model_width):
    quarter = model_width // 4
    omegas = jnp.power(10000.0, -jnp.arange(quarter, dtype=jnp.float32) / quarter)
    row_angle = positions[0].astype(jnp.float32)[:, None] * omegas[None, :]
    col_angle = positions[1].astype(jnp.float32)[:, None] * omegas[None, :]
    return jnp.concatenate(
        [jnp.sin(row_angle), jnp.cos(row_angle), jnp.sin(col_angle), jnp.cos(col_angle)], axis=1
    )


def attend_update(running, query_heads, key_piece, value_piece, mask_piece, inv_root):
    row_top, denominator, weighted = running
    key_count = key_piece.shape[0]
    head_count = query_heads.shape[1]
    head_size = query_heads.shape[2]
    key_heads = key_piece.reshape(key_count, head_count, head_size)
    value_heads = value_piece.reshape(key_count, head_count, head_size)
    scores = (
        jnp.einsum("qhd,khd->hqk", query_heads, key_heads, preferred_element_type=jnp.float32)
        * inv_root
    )
    scores = jnp.where(mask_piece[None, None, :], scores, neg_large)
    new_top = jnp.maximum(row_top, jnp.max(scores, axis=2))
    weights = jnp.where(mask_piece[None, None, :], jnp.exp(scores - new_top[:, :, None]), 0.0)
    factor = jnp.exp(row_top - new_top)
    denominator = denominator * factor + jnp.sum(weights, axis=2)
    rounded = weights.astype(jnp.bfloat16)
    weighted = weighted * factor[:, :, None] + jnp.einsum(
        "hqk,khd->hqd", rounded, value_heads, preferred_element_type=jnp.float32
    )
    return (new_top, denominator, weighted)


def make_folder(query_heads, key_valid, inv_root):

    def fold_keys(running, shard_piece, start_row):
        key_piece, value_piece = shard_piece
        key_count = key_piece.shape[0]
        if key_count > 2 * key_block and key_count % key_block == 0:
            block_total = key_count // key_block

            def block_step(carried, block_items):
                return (
                    attend_update(
                        carried,
                        query_heads,
                        block_items[0],
                        block_items[1],
                        block_items[2],
                        inv_root,
                    ),
                    None,
                )

            stacked = (
                key_piece.reshape(block_total, key_block, key_piece.shape[1]),
                value_piece.reshape(block_total, key_block, value_piece.shape[1]),
                key_valid.reshape(block_total, key_block),
            )
            running, unused = lax.scan(block_step, running, stacked)
            return running
        return attend_update(running, query_heads, key_piece, value_piece, key_valid, inv_root)

    return fold_keys


def initial_state(query_rows, head_count, head_size):
    return (
        jnp.full((head_count, query_rows), neg_large, jnp.float32),
        jnp.zeros((head_count, query_rows), jnp.float32),
        jnp.zeros((head_count, query_rows, head_size), jnp.float32),
    )


def finish_state(running):
    row_top, denominator, weighted = running
    normalized = weighted / denominator[:, :, None]
    head_count, query_rows, head_size = normalized.shape
    return (
        jnp.transpose(normalized, (1, 0, 2))
        .reshape(query_rows, head_count * head_size)
        .astype(jnp.bfloat16)
    )


def per_device(
    tokens, positions, counts, timestep, time_in, time_out, ada_weight, qkv_weight, out_weight
):
    devices = lax.axis_size("patch")
    my_index = lax.axis_index("patch")
    local_rows = tokens.shape[0]
    model_width = tokens.shape[1]
    head_count = HEADS
    head_size = model_width // head_count
    inv_root = 1.0 / math.sqrt(head_size)
    features = time_features(timestep, time_in.shape[0])
    hidden_time = jax.nn.silu(
        jnp.dot(features, time_in, preferred_element_type=jnp.float32)
    ).astype(jnp.bfloat16)
    cond_part = jnp.dot(hidden_time, time_out, preferred_element_type=jnp.float32)
    activated = jax.nn.silu(cond_part).astype(jnp.bfloat16)
    partial_mod = jnp.dot(activated, ada_weight, preferred_element_type=jnp.float32)
    modulation = jnp.sum(lax.all_gather(partial_mod[0], "patch"), axis=0, keepdims=True)
    shift_mod = modulation[:, :model_width]
    scale_mod = modulation[:, model_width : 2 * model_width]
    gate_mod = modulation[:, 2 * model_width :]
    x_in = tokens.astype(jnp.float32) + position_table(positions, model_width)
    mean_value = jnp.mean(x_in, axis=1, keepdims=True)
    centered = x_in - mean_value
    variance = jnp.mean(centered * centered, axis=1, keepdims=True)
    normed = centered * lax.rsqrt(variance + 1e-06)
    modulated = (normed * (1.0 + scale_mod) + shift_mod).astype(jnp.bfloat16)
    counts_here = lax.dynamic_index_in_dim(counts, my_index, keepdims=False)
    row_ids = jnp.arange(local_rows, dtype=jnp.int32)
    row_valid = row_ids < counts_here
    projections = jnp.dot(modulated, qkv_weight, preferred_element_type=jnp.float32).astype(
        jnp.bfloat16
    )
    groups = devices // head_count
    part_rows = local_rows // groups
    query_split = projections[:, :model_width].reshape(groups, part_rows, head_count, head_size)
    query_send = jnp.transpose(query_split, (0, 2, 1, 3)).reshape(devices, part_rows, head_size)
    key_split = projections[:, model_width : 2 * model_width].reshape(
        local_rows, head_count, head_size
    )
    value_split = projections[:, 2 * model_width :].reshape(local_rows, head_count, head_size)
    pair_heads = jnp.transpose(jnp.concatenate([key_split, value_split], axis=2), (1, 0, 2))
    pair_send = jnp.broadcast_to(pair_heads[None], (groups, head_count, local_rows, 2 * head_size))
    pair_send = pair_send.reshape(devices, local_rows, 2 * head_size)
    got_query, got_pair = (
        lax.all_to_all(query_send, "patch", split_axis=0, concat_axis=0, tiled=True),
        lax.all_to_all(pair_send, "patch", split_axis=0, concat_axis=0, tiled=True),
    )
    query_rows = devices * part_rows
    query_heads = got_query.reshape(query_rows, 1, head_size)
    all_pairs = got_pair.reshape(devices * local_rows, 2 * head_size)
    key_valid = (jnp.arange(local_rows, dtype=jnp.int32)[None, :] < counts[:, None]).reshape(-1)
    folder = make_folder(query_heads, key_valid, inv_root)
    running = folder(
        initial_state(query_rows, 1, head_size),
        (all_pairs[:, :head_size], all_pairs[:, head_size:]),
        0,
    )
    head_result = finish_state(running).reshape(devices, part_rows, head_size)
    came_back = lax.all_to_all(head_result, "patch", split_axis=0, concat_axis=0, tiled=True)
    attended = jnp.transpose(
        came_back.reshape(groups, head_count, part_rows, head_size), (0, 2, 1, 3)
    )
    attended = attended.reshape(local_rows, model_width)
    projected = jnp.dot(attended, out_weight, preferred_element_type=jnp.float32)
    valid_column = row_valid.astype(jnp.float32)[:, None]
    return (x_in + gate_mod * projected * valid_column).astype(jnp.bfloat16)


def solution(mesh):
    placed = (
        P(("req", "patch"), None),
        P(None, ("req", "patch")),
        P("req"),
        P("req"),
        P(),
        P(None, "patch"),
        P("patch", None),
        P(),
        P(),
    )
    return jax.shard_map(
        per_device, mesh=mesh, in_specs=placed, out_specs=P(("req", "patch"), None), check_vma=False
    )
```

```python
import functools
import math

import jax
import jax.numpy as jnp
import numpy as np
from jax import lax
from jax.experimental import pallas as pl
from jax.experimental.pallas import tpu as pltpu
from jax.sharding import PartitionSpec as P

HEADS = 16
NEG = -1e30
F32 = jnp.float32
BF16 = jnp.bfloat16
MESH = pl.DeviceIdType.MESH


def silu(v):
    return v / (1.0 + jnp.exp(-v))


def dot(a, b):
    return jnp.dot(a, b, preferred_element_type=F32)


def one_row_dot(row, matrix):
    wide = jnp.broadcast_to(row, (16, row.shape[1])).astype(BF16)
    return dot(wide, matrix)[0:1]


def block_kernel(
    n, rows, width, head,
    counts, tstep, pos, pos_tab, time_tab,
    tok_h, tin_h, tout_h, ada_h, qkv_h, ow_h,
    out,
    tok, tin, tout, ada, qkv, ow, mods, xin_s, norm_s, send, got, kbuf, vbuf, att, back,
    lsem, wsem, msend, mrecv, psend, precv, asend, arecv,
):
    me = lax.axis_index("patch")
    my_head = lax.rem(me, HEADS)
    group = me // HEADS
    chunk = HEADS * rows
    groups = n // HEADS
    inv_root = 1.0 / math.sqrt(head)

    barrier = pltpu.get_barrier_semaphore()

    @pl.loop(1, n)
    def _(step):
        pl.semaphore_signal(
            barrier, inc=1, device_id={"patch": lax.rem(me + step, n)}, device_id_type=MESH
        )

    loads = [
        pltpu.make_async_copy(src, dst, lsem.at[i])
        for i, (src, dst) in enumerate(
            [(tin_h, tin), (tout_h, tout), (ada_h, ada), (tok_h, tok), (qkv_h, qkv)]
        )
    ]
    for load in loads:
        load.start()
    ow[:, head:, :] = jnp.zeros((HEADS, ow.shape[1] - head, width), BF16)
    ow_loads = [
        pltpu.make_async_copy(
            ow_h.at[pl.ds(h * head, head), :], ow.at[h, pl.ds(0, head), :], wsem.at[h]
        )
        for h in range(HEADS)
    ]
    for load in ow_loads:
        load.start()

    angles = tstep[0].astype(F32) * time_tab[0:1, :] + time_tab[1:2, :]
    features = jnp.sin(angles).astype(BF16)
    loads[0].wait()
    hidden = silu(one_row_dot(features, tin[...])).astype(BF16)
    loads[1].wait()
    activated = silu(one_row_dot(hidden, tout[...])).astype(BF16)
    loads[2].wait()
    mods[me] = one_row_dot(activated, ada[...])

    pl.semaphore_wait(barrier, n - 1)

    def mod_copy(step, slot):
        return pltpu.make_async_remote_copy(
            src_ref=mods.at[slot],
            dst_ref=mods.at[slot],
            send_sem=msend.at[step],
            recv_sem=mrecv.at[slot],
            device_id={"patch": lax.rem(me + step, n)},
            device_id_type=MESH,
        )

    @pl.loop(1, n)
    def _(step):
        mod_copy(step, me).start()

    ids = lax.broadcasted_iota(jnp.int32, (rows, rows), 0)
    eye = ids == lax.broadcasted_iota(jnp.int32, (rows, rows), 1)
    posf = pos[...].astype(F32)
    row_col = jnp.sum(jnp.where(eye, posf[0:1, :], 0.0), axis=1, keepdims=True)
    col_col = jnp.sum(jnp.where(eye, posf[1:2, :], 0.0), axis=1, keepdims=True)
    lanes = lax.broadcasted_iota(jnp.int32, (1, width), 1)
    first = lanes < width // 2
    place = jnp.where(first, row_col, col_col)
    embed = jnp.sin(place * pos_tab[0:1, :] + pos_tab[1:2, :])
    loads[3].wait()
    x_in = tok[...].astype(F32) + embed
    xin_s[...] = x_in
    centered = x_in - jnp.mean(x_in, axis=1, keepdims=True)
    variance = jnp.mean(centered * centered, axis=1, keepdims=True)
    norm_s[...] = centered * lax.rsqrt(variance + 1e-6)

    @pl.loop(1, n)
    def _(step):
        mod_copy(step, lax.rem(me - step + n, n)).wait_recv()

    modulation = jnp.sum(mods[...], axis=0)
    shift = modulation[:, :width]
    scale = modulation[:, width : 2 * width]
    gate = modulation[:, 2 * width :]
    modulated = (norm_s[...] * (1.0 + scale) + shift).astype(BF16)
    loads[4].wait()
    parts = [
        dot(modulated, qkv[:, i * width : (i + 1) * width]).astype(BF16) for i in range(3)
    ]
    spare = jnp.zeros((rows, send.shape[2] - 3 * head), BF16)
    for h in range(HEADS):
        cols = slice(h * head, (h + 1) * head)
        send[h] = jnp.concatenate([part[:, cols] for part in parts] + [spare], axis=1)

    def pair_copy(step, slot):
        to = lax.rem(me + step, n)
        return pltpu.make_async_remote_copy(
            src_ref=send.at[lax.rem(to, HEADS)],
            dst_ref=got.at[slot],
            send_sem=psend.at[step],
            recv_sem=precv.at[slot],
            device_id={"patch": to},
            device_id_type=MESH,
        )

    @pl.loop(1, n)
    def _(step):
        pair_copy(step, me).start()

    got[me] = send[my_head]
    vbuf[...] = jnp.zeros(vbuf.shape, BF16)

    @pl.loop(1, n)
    def _(step):
        pair_copy(step, lax.rem(me - step + n, n)).wait_recv()

    for g in range(groups):
        block = got[g * HEADS : (g + 1) * HEADS].reshape(chunk, got.shape[2])
        kbuf[g * chunk : (g + 1) * chunk, :] = block[:, head : 2 * head]
        vbuf[g * chunk : (g + 1) * chunk, :head] = block[:, 2 * head : 3 * head]

    def mask_of(g):
        slots = lax.broadcasted_iota(jnp.int32, (1, chunk), 1)
        bias = jnp.full((1, chunk), NEG, F32)
        for b in range(HEADS):
            inside = (slots >= b * rows) & (slots < b * rows + counts[g * HEADS + b])
            bias = jnp.where(inside, 0.0, bias)
        return bias

    masks = [mask_of(g) for g in range(groups)]

    def att_copy(j, slot, to):
        return pltpu.make_async_remote_copy(
            src_ref=att.at[j],
            dst_ref=back.at[slot],
            send_sem=asend.at[j],
            recv_sem=arecv.at[slot],
            device_id={"patch": group * HEADS + to},
            device_id_type=MESH,
        )

    pairs = 2

    @pl.loop(0, HEADS // pairs)
    def _(step):
        base = lax.rem(my_head // pairs + 1 + step, HEADS // pairs) * pairs
        block = got[pl.ds(group * HEADS + base, pairs)].reshape(pairs * rows, got.shape[2])
        query = block[:, :head]
        top = total = weighted = None
        for g in range(groups):
            keys = kbuf[g * chunk : (g + 1) * chunk, :]
            scores = lax.dot_general(
                query, keys, (((1,), (1,)), ((), ())), preferred_element_type=F32
            )
            scores = scores * inv_root + masks[g]
            new_top = jnp.max(scores, axis=1, keepdims=True)
            if g:
                new_top = jnp.maximum(top, new_top)
            prob = jnp.exp(scores - new_top)
            mass = jnp.sum(prob, axis=1, keepdims=True)
            mixed = dot(prob.astype(BF16), vbuf[g * chunk : (g + 1) * chunk, :])
            if g:
                factor = jnp.exp(top - new_top)
                mass = total * factor + mass
                mixed = weighted * factor + mixed
            top, total, weighted = new_top, mass, mixed
        att[pl.ds(base, pairs)] = (
            (weighted / total).astype(BF16).reshape(pairs, rows, att.shape[2])
        )
        for i in range(pairs):

            @pl.when(base + i != my_head)
            def _():
                att_copy(base + i, my_head, base + i).start()

    back[my_head] = att[my_head]
    for load in ow_loads:
        load.wait()

    @pl.loop(1, HEADS)
    def _(step):
        other = lax.rem(my_head + step, HEADS)
        att_copy(other, other, other).wait_recv()

    attended = jnp.concatenate([back[h] for h in range(HEADS)], axis=1)
    projected = dot(attended, ow[...].reshape(HEADS * ow.shape[1], width))
    valid = (lax.broadcasted_iota(jnp.int32, (rows, 1), 0) < counts[me]).astype(F32)
    out[...] = (xin_s[...] + gate * projected * valid).astype(BF16)

    @pl.loop(1, n)
    def _(step):
        mod_copy(step, me).wait_send()
        pair_copy(step, me).wait_send()

    @pl.loop(1, HEADS)
    def _(step):
        other = lax.rem(my_head + step, HEADS)
        att_copy(other, other, other).wait_send()


def tables(width, freq):
    quarter, half = width // 4, freq // 2
    omega = np.power(10000.0, -np.arange(quarter) / quarter)
    turn = math.pi / 2
    pos_tab = np.stack([np.tile(omega, 4), np.repeat([0.0, turn, 0.0, turn], quarter)])
    wave = np.exp(-math.log(10000.0) * np.arange(half) / half)
    time_tab = np.stack([np.tile(wave, 2), np.repeat([turn, 0.0], half)])
    return pos_tab.astype(np.float32), time_tab.astype(np.float32)


def per_device(
    tokens, positions, counts, timestep, time_in, time_out, ada_weight, qkv_weight, out_weight
):
    n = lax.axis_size("patch")
    rows, width = tokens.shape
    head = width // HEADS
    lane = 128
    head_pad = -(-head // lane) * lane
    pack = -(-3 * head // lane) * lane
    pos_tab, time_tab = tables(width, time_in.shape[0])
    smem = pl.BlockSpec(memory_space=pltpu.SMEM)
    vmem = pl.BlockSpec(memory_space=pltpu.VMEM)
    hbm = pl.BlockSpec(memory_space=pl.ANY)
    return pl.pallas_call(
        functools.partial(block_kernel, n, rows, width, head),
        out_shape=jax.ShapeDtypeStruct((rows, width), BF16),
        in_specs=[smem, smem, vmem, vmem, vmem] + [hbm] * 6,
        out_specs=vmem,
        scratch_shapes=[
            pltpu.VMEM(tokens.shape, BF16),
            pltpu.VMEM(time_in.shape, BF16),
            pltpu.VMEM(time_out.shape, BF16),
            pltpu.VMEM(ada_weight.shape, BF16),
            pltpu.VMEM(qkv_weight.shape, BF16),
            pltpu.VMEM((HEADS, head_pad, width), BF16),
            pltpu.VMEM((n, 1, 3 * width), F32),
            pltpu.VMEM((rows, width), F32),
            pltpu.VMEM((rows, width), F32),
            pltpu.VMEM((HEADS, rows, pack), BF16),
            pltpu.VMEM((n, rows, pack), BF16),
            pltpu.VMEM((n * rows, head), BF16),
            pltpu.VMEM((n * rows, head_pad), BF16),
            pltpu.VMEM((HEADS, rows, head_pad), BF16),
            pltpu.VMEM((HEADS, rows, head_pad), BF16),
            pltpu.SemaphoreType.DMA((5,)),
            pltpu.SemaphoreType.DMA((HEADS,)),
            pltpu.SemaphoreType.DMA((n,)),
            pltpu.SemaphoreType.DMA((n,)),
            pltpu.SemaphoreType.DMA((n,)),
            pltpu.SemaphoreType.DMA((n,)),
            pltpu.SemaphoreType.DMA((HEADS,)),
            pltpu.SemaphoreType.DMA((HEADS,)),
        ],
        compiler_params=pltpu.CompilerParams(
            collective_id=0, has_side_effects=True, vmem_limit_bytes=60 * 2**20
        ),
    )(
        counts, timestep, positions, pos_tab, time_tab,
        tokens, time_in, time_out, ada_weight, qkv_weight, out_weight,
    )


def solution(mesh):
    placed = (
        P(("req", "patch"), None),
        P(None, ("req", "patch")),
        P("req"),
        P("req"),
        P(),
        P(None, "patch"),
        P("patch", None),
        P(),
        P(),
    )
    return jax.shard_map(
        per_device, mesh=mesh, in_specs=placed, out_specs=P(("req", "patch"), None), check_vma=False
    )
```

```python
import functools
import math

import jax
import jax.numpy as jnp
import numpy as np
from jax import lax
from jax.experimental import pallas as pl
from jax.experimental.pallas import tpu as pltpu
from jax.sharding import PartitionSpec as P

HEADS = 16
NEG = -1e30
F32 = jnp.float32
BF16 = jnp.bfloat16
MESH = pl.DeviceIdType.MESH


def silu(v):
    return v / (1.0 + jnp.exp(-v))


def dot(a, b):
    return jnp.dot(a, b, preferred_element_type=F32)


def one_row_dot(row, matrix):
    wide = jnp.broadcast_to(row, (16, row.shape[1])).astype(BF16)
    return dot(wide, matrix)[0:1]


def block_kernel(
    n, rows, width, head,
    counts, tstep, pos, pos_tab, time_tab,
    tok_h, tin_h, tout_h, ada_h, qkv_h, ow_h,
    out,
    tok, tin, tout, ada, qkv, ow, mods, gates, xin_s, norm_s, send, got, kbuf, vbuf, att, back,
    lsem, wsem, msend, mrecv, gsend, grecv, psend, precv, asend, arecv,
):
    me = lax.axis_index("patch")
    my_head = lax.rem(me, HEADS)
    group = me // HEADS
    chunk = HEADS * rows
    groups = n // HEADS
    inv_root = math.log2(math.e) / math.sqrt(head)

    barrier = pltpu.get_barrier_semaphore()

    @pl.loop(1, n)
    def _(step):
        pl.semaphore_signal(
            barrier, inc=1, device_id={"patch": lax.rem(me + step, n)}, device_id_type=MESH
        )

    loads = [
        pltpu.make_async_copy(src, dst, lsem.at[i])
        for i, (src, dst) in enumerate(
            [(tin_h, tin), (tout_h, tout), (ada_h, ada), (tok_h, tok), (qkv_h, qkv)]
        )
    ]
    for load in loads:
        load.start()
    ow[:, head:, :] = jnp.zeros((HEADS, ow.shape[1] - head, width), BF16)
    ow_loads = [
        pltpu.make_async_copy(
            ow_h.at[pl.ds(h * head, head), :], ow.at[h, pl.ds(0, head), :], wsem.at[h]
        )
        for h in range(HEADS)
    ]
    for load in ow_loads:
        load.start()

    angles = tstep[0].astype(F32) * time_tab[0:1, :] + time_tab[1:2, :]
    features = jnp.sin(angles).astype(BF16)
    loads[0].wait()
    hidden = silu(one_row_dot(features, tin[...])).astype(BF16)
    loads[1].wait()
    wide = jnp.broadcast_to(hidden, (16, width))
    cond = lax.dot_general(wide, tout[...], (((1,), (1,)), ((), ())), preferred_element_type=F32)
    activated = silu(cond[0:1]).astype(BF16)
    loads[2].wait()
    partial = one_row_dot(activated, ada[...])
    mods[me] = jnp.concatenate(
        [partial[:, :width], partial[:, width : 2 * width]], axis=0
    ).astype(BF16)
    gates[me] = partial[:, 2 * width :]

    pl.semaphore_wait(barrier, n - 1)

    def mod_copy(step, slot):
        return pltpu.make_async_remote_copy(
            src_ref=mods.at[slot],
            dst_ref=mods.at[slot],
            send_sem=msend.at[step],
            recv_sem=mrecv.at[slot],
            device_id={"patch": lax.rem(me + step, n)},
            device_id_type=MESH,
        )

    def gate_copy(step, slot):
        return pltpu.make_async_remote_copy(
            src_ref=gates.at[slot],
            dst_ref=gates.at[slot],
            send_sem=gsend.at[step],
            recv_sem=grecv.at[slot],
            device_id={"patch": lax.rem(me + step, n)},
            device_id_type=MESH,
        )

    @pl.loop(1, n)
    def _(step):
        mod_copy(step, me).start()

    ids = lax.broadcasted_iota(jnp.int32, (rows, rows), 0)
    eye = ids == lax.broadcasted_iota(jnp.int32, (rows, rows), 1)
    posf = pos[...].astype(F32)
    row_col = jnp.sum(jnp.where(eye, posf[0:1, :], 0.0), axis=1, keepdims=True)
    col_col = jnp.sum(jnp.where(eye, posf[1:2, :], 0.0), axis=1, keepdims=True)
    lanes = lax.broadcasted_iota(jnp.int32, (1, width), 1)
    first = lanes < width // 2
    place = jnp.where(first, row_col, col_col)
    embed = jnp.sin(place * pos_tab[0:1, :] + pos_tab[1:2, :])
    loads[3].wait()
    x_in = tok[...].astype(F32) + embed
    xin_s[...] = x_in
    centered = x_in - jnp.mean(x_in, axis=1, keepdims=True)
    variance = jnp.mean(centered * centered, axis=1, keepdims=True)
    norm_s[...] = centered * lax.rsqrt(variance + 1e-6)

    @pl.loop(1, n)
    def _(step):
        mod_copy(step, lax.rem(me - step + n, n)).wait_recv()

    modulation = jnp.sum(mods[...].astype(F32), axis=0)
    shift = modulation[0:1]
    scale = modulation[1:2]
    modulated = (norm_s[...] * (1.0 + scale) + shift).astype(BF16)
    loads[4].wait()
    parts = [
        dot(modulated, qkv[:, i * width : (i + 1) * width]).astype(BF16) for i in range(3)
    ]
    spare = jnp.zeros((rows, send.shape[2] - 3 * head), BF16)
    for h in range(HEADS):
        cols = slice(h * head, (h + 1) * head)
        send[h] = jnp.concatenate([part[:, cols] for part in parts] + [spare], axis=1)

    def pair_copy(step, slot):
        to = lax.rem(me + step, n)
        return pltpu.make_async_remote_copy(
            src_ref=send.at[lax.rem(to, HEADS)],
            dst_ref=got.at[slot],
            send_sem=psend.at[step],
            recv_sem=precv.at[slot],
            device_id={"patch": to},
            device_id_type=MESH,
        )

    @pl.loop(1, n)
    def _(step):
        pair_copy(step, me).start()

    got[me] = send[my_head]
    tail = lax.broadcasted_iota(jnp.int32, (chunk, vbuf.shape[1] - head), 1)
    ones = jnp.where(tail == 0, 1.0, 0.0).astype(BF16)
    slot_ids = lax.broadcasted_iota(jnp.int32, (rows, 1), 0)
    lane_ids = lax.broadcasted_iota(jnp.int32, (rows, kbuf.shape[1]), 1)
    for g in range(groups):
        vbuf[g * chunk : (g + 1) * chunk, head:] = ones
    for b in range(n):
        bias = jnp.where(slot_ids < counts[b], 0.0, NEG)
        kbuf[b * rows : (b + 1) * rows, :] = jnp.where(lane_ids == head, bias, 0.0).astype(BF16)

    @pl.loop(1, n)
    def _(step):
        pair_copy(step, lax.rem(me - step + n, n)).wait_recv()

    @pl.loop(1, n)
    def _(step):
        gate_copy(step, me).start()


    for g in range(groups):
        block = got[g * HEADS : (g + 1) * HEADS].reshape(chunk, got.shape[2])
        kbuf[g * chunk : (g + 1) * chunk, :head] = block[:, head : 2 * head]
        vbuf[g * chunk : (g + 1) * chunk, :head] = block[:, 2 * head : 3 * head]


    def att_copy(j, slot, to):
        return pltpu.make_async_remote_copy(
            src_ref=att.at[j],
            dst_ref=back.at[slot],
            send_sem=asend.at[j],
            recv_sem=arecv.at[slot],
            device_id={"patch": group * HEADS + to},
            device_id_type=MESH,
        )

    pairs = 2

    @pl.loop(0, HEADS // pairs)
    def _(step):
        base = lax.rem(my_head // pairs + 1 + step, HEADS // pairs) * pairs
        block = got[pl.ds(group * HEADS + base, pairs)].reshape(pairs * rows, got.shape[2])
        query = jnp.concatenate(
            [block[:, :head], jnp.ones((pairs * rows, 1), BF16)], axis=1
        )
        query = jnp.concatenate(
            [query, jnp.zeros((pairs * rows, kbuf.shape[1] - head - 1), BF16)], axis=1
        )
        top = weighted = None
        for g in range(groups):
            keys = kbuf[g * chunk : (g + 1) * chunk, :]
            scores = lax.dot_general(
                query, keys, (((1,), (1,)), ((), ())), preferred_element_type=F32
            )
            new_top = jnp.max(scores, axis=1, keepdims=True)
            if g:
                new_top = jnp.maximum(top, new_top)
            prob = jnp.exp2((scores - new_top) * inv_root).astype(BF16)
            mixed = dot(prob, vbuf[g * chunk : (g + 1) * chunk, :])
            if g:
                mixed = weighted * jnp.exp2((top - new_top) * inv_root) + mixed
            top, weighted = new_top, mixed
        total = weighted[:, head : head + 1]
        att[pl.ds(base, pairs)] = (
            (weighted / total).astype(BF16).reshape(pairs, rows, att.shape[2])
        )
        for i in range(pairs):

            @pl.when(base + i != my_head)
            def _():
                att_copy(base + i, my_head, base + i).start()

    back[my_head] = att[my_head]
    for load in ow_loads:
        load.wait()

    @pl.loop(1, HEADS)
    def _(step):
        other = lax.rem(my_head + step, HEADS)
        att_copy(other, other, other).wait_recv()

    @pl.loop(1, n)
    def _(step):
        gate_copy(step, lax.rem(me - step + n, n)).wait_recv()

    gate = jnp.sum(gates[...], axis=0)
    attended = jnp.concatenate([back[h] for h in range(HEADS)], axis=1)
    projected = dot(attended, ow[...].reshape(HEADS * ow.shape[1], width))
    valid = (lax.broadcasted_iota(jnp.int32, (rows, 1), 0) < counts[me]).astype(F32)
    out[...] = xin_s[...] + gate * projected * valid

    @pl.loop(1, n)
    def _(step):
        mod_copy(step, me).wait_send()
        pair_copy(step, me).wait_send()
        gate_copy(step, me).wait_send()

    @pl.loop(1, HEADS)
    def _(step):
        other = lax.rem(my_head + step, HEADS)
        att_copy(other, other, other).wait_send()


def tables(width, freq):
    quarter, half = width // 4, freq // 2
    omega = np.power(10000.0, -np.arange(quarter) / quarter)
    turn = math.pi / 2
    pos_tab = np.stack([np.tile(omega, 4), np.repeat([0.0, turn, 0.0, turn], quarter)])
    wave = np.exp(-math.log(10000.0) * np.arange(half) / half)
    time_tab = np.stack([np.tile(wave, 2), np.repeat([turn, 0.0], half)])
    return pos_tab.astype(np.float32), time_tab.astype(np.float32)


def per_device(
    tokens, positions, counts, timestep, time_in, time_out, ada_weight, qkv_weight, out_weight
):
    n = lax.axis_size("patch")
    rows, width = tokens.shape
    head = width // HEADS
    lane = 128
    head_pad = -(-head // lane) * lane
    pack = -(-3 * head // lane) * lane
    pos_tab, time_tab = tables(width, time_in.shape[0])
    smem = pl.BlockSpec(memory_space=pltpu.SMEM)
    vmem = pl.BlockSpec(memory_space=pltpu.VMEM)
    hbm = pl.BlockSpec(memory_space=pl.ANY)
    result = pl.pallas_call(
        functools.partial(block_kernel, n, rows, width, head),
        out_shape=jax.ShapeDtypeStruct((rows, width), F32),
        in_specs=[smem, smem, vmem, vmem, vmem] + [hbm] * 6,
        out_specs=vmem,
        scratch_shapes=[
            pltpu.VMEM(tokens.shape, BF16),
            pltpu.VMEM(time_in.shape, BF16),
            pltpu.VMEM(time_out.shape[::-1], BF16),
            pltpu.VMEM(ada_weight.shape, BF16),
            pltpu.VMEM(qkv_weight.shape, BF16),
            pltpu.VMEM((HEADS, head_pad, width), BF16),
            pltpu.VMEM((n, 2, width), BF16),
            pltpu.VMEM((n, 1, width), F32),
            pltpu.VMEM((rows, width), F32),
            pltpu.VMEM((rows, width), F32),
            pltpu.VMEM((HEADS, rows, pack), BF16),
            pltpu.VMEM((n, rows, pack), BF16),
            pltpu.VMEM((n * rows, head_pad), BF16),
            pltpu.VMEM((n * rows, head_pad), BF16),
            pltpu.VMEM((HEADS, rows, head_pad), BF16),
            pltpu.VMEM((HEADS, rows, head_pad), BF16),
            pltpu.SemaphoreType.DMA((5,)),
            pltpu.SemaphoreType.DMA((HEADS,)),
            pltpu.SemaphoreType.DMA((n,)),
            pltpu.SemaphoreType.DMA((n,)),
            pltpu.SemaphoreType.DMA((n,)),
            pltpu.SemaphoreType.DMA((n,)),
            pltpu.SemaphoreType.DMA((n,)),
            pltpu.SemaphoreType.DMA((n,)),
            pltpu.SemaphoreType.DMA((HEADS,)),
            pltpu.SemaphoreType.DMA((HEADS,)),
        ],
        compiler_params=pltpu.CompilerParams(
            collective_id=0, has_side_effects=True, vmem_limit_bytes=60 * 2**20
        ),
    )(
        counts, timestep, positions, pos_tab, time_tab,
        tokens, time_in, time_out.T, ada_weight, qkv_weight, out_weight,
    )
    return result.astype(BF16)


def solution(mesh):
    placed = (
        P(("req", "patch"), None),
        P(None, ("req", "patch")),
        P("req"),
        P("req"),
        P(),
        P(None, "patch"),
        P("patch", None),
        P(),
        P(),
    )
    return jax.shard_map(
        per_device, mesh=mesh, in_specs=placed, out_specs=P(("req", "patch"), None), check_vma=False
    )
```

```python
import functools
import math

import jax
import jax.numpy as jnp
import numpy as np
from jax import lax
from jax.experimental import pallas as pl
from jax.experimental.pallas import tpu as pltpu
from jax.sharding import PartitionSpec as P

HEADS = 16
NEG = -1e30
F32 = jnp.float32
BF16 = jnp.bfloat16
MESH = pl.DeviceIdType.MESH


def silu(v):
    return v / (1.0 + jnp.exp(-v))


def dot(a, b):
    return jnp.dot(a, b, preferred_element_type=F32)


def one_row_dot(row, matrix):
    wide = jnp.broadcast_to(row, (16, row.shape[1])).astype(BF16)
    return dot(wide, matrix)[0:1]


def fold_group(rows, extra):
    group = 8
    while rows // group * extra > 128:
        group *= 2
    return group


def fold(block):
    rows, extra = block.shape[0], block.shape[1] - 64
    group = fold_group(rows, extra)
    half = rows // 2
    main = jnp.concatenate([block[:half, :64], block[half:, :64]], axis=1)
    pieces = [block[r : r + group, 64:] for r in range(0, rows, group)]
    spare = 128 - extra * len(pieces)
    rest = jnp.concatenate(pieces + [jnp.zeros((group, spare), F32)], axis=1)
    return jnp.concatenate([main, rest], axis=0)


def unfold(packed, rows, extra):
    half = rows // 2
    left = jnp.concatenate([packed[:half, :64], packed[:half, 64:]], axis=0)
    rest = packed[half:]
    count = rows // fold_group(rows, extra)
    right = jnp.concatenate([rest[:, r * extra : (r + 1) * extra] for r in range(count)], axis=0)
    return jnp.concatenate([left, right], axis=1)


def block_kernel(
    n, rows, width, head,
    counts, tstep, pos, pos_tab, time_tab,
    tok_h, tin_h, tout_h, ada_h, qkv_h, ow_h,
    out,
    tok, tin, tout, ada, qkv, ow, mods, gates, xin_s, norm_s, send, got, kbuf, vbuf, att, back,
    lsem, wsem, msend, mrecv, gsend, grecv, psend, precv, asend, arecv,
):
    me = lax.axis_index("patch")
    my_head = lax.rem(me, HEADS)
    group = me // HEADS
    chunk = HEADS * rows
    groups = n // HEADS
    inv_root = math.log2(math.e) / math.sqrt(head)

    barrier = pltpu.get_barrier_semaphore()

    @pl.loop(1, n)
    def _(step):
        pl.semaphore_signal(
            barrier, inc=1, device_id={"patch": lax.rem(me + step, n)}, device_id_type=MESH
        )

    loads = [
        pltpu.make_async_copy(src, dst, lsem.at[i])
        for i, (src, dst) in enumerate(
            [(tin_h, tin), (tout_h, tout), (ada_h, ada), (tok_h, tok), (qkv_h, qkv)]
        )
    ]
    for load in loads[:3]:
        load.start()

    angles = tstep[0].astype(F32) * time_tab[0:1, :] + time_tab[1:2, :]
    features = jnp.sin(angles).astype(BF16)
    loads[0].wait()
    hidden = silu(one_row_dot(features, tin[...])).astype(BF16)
    loads[1].wait()
    wide = jnp.broadcast_to(hidden, (16, width))
    cond = lax.dot_general(wide, tout[...], (((1,), (1,)), ((), ())), preferred_element_type=F32)
    activated = silu(cond[0:1]).astype(BF16)
    loads[2].wait()
    partial = one_row_dot(activated, ada[...])
    mods[me] = jnp.concatenate(
        [partial[:, :width], partial[:, width : 2 * width]], axis=0
    ).astype(BF16)
    span = gates.shape[2]
    gates[me] = jnp.concatenate(
        [partial[:, 2 * width : 2 * width + span], partial[:, 3 * width - span :]], axis=0
    ).astype(BF16)
    for load in loads[3:]:
        load.start()

    pl.semaphore_wait(barrier, n - 1)

    def mod_copy(step, slot):
        return pltpu.make_async_remote_copy(
            src_ref=mods.at[slot],
            dst_ref=mods.at[slot],
            send_sem=msend.at[step],
            recv_sem=mrecv.at[slot],
            device_id={"patch": lax.rem(me + step, n)},
            device_id_type=MESH,
        )

    def gate_copy(step, slot):
        return pltpu.make_async_remote_copy(
            src_ref=gates.at[slot],
            dst_ref=gates.at[slot],
            send_sem=gsend.at[step],
            recv_sem=grecv.at[slot],
            device_id={"patch": lax.rem(me + step, n)},
            device_id_type=MESH,
        )

    @pl.loop(1, n)
    def _(step):
        mod_copy(step, me).start()

    ow[:, head:, :] = jnp.zeros((HEADS, ow.shape[1] - head, width), BF16)
    ow_loads = [
        pltpu.make_async_copy(
            ow_h.at[pl.ds(h * head, head), :], ow.at[h, pl.ds(0, head), :], wsem.at[h]
        )
        for h in range(HEADS)
    ]
    for load in ow_loads:
        load.start()

    ids = lax.broadcasted_iota(jnp.int32, (rows, rows), 0)
    eye = ids == lax.broadcasted_iota(jnp.int32, (rows, rows), 1)
    posf = pos[...].astype(F32)
    row_col = jnp.sum(jnp.where(eye, posf[0:1, :], 0.0), axis=1, keepdims=True)
    col_col = jnp.sum(jnp.where(eye, posf[1:2, :], 0.0), axis=1, keepdims=True)
    lanes = lax.broadcasted_iota(jnp.int32, (1, width), 1)
    first = lanes < width // 2
    place = jnp.where(first, row_col, col_col)
    embed = jnp.sin(place * pos_tab[0:1, :] + pos_tab[1:2, :])
    loads[3].wait()
    x_in = tok[...].astype(F32) + embed
    xin_s[...] = x_in
    centered = x_in - jnp.mean(x_in, axis=1, keepdims=True)
    variance = jnp.mean(centered * centered, axis=1, keepdims=True)
    norm_s[...] = centered * lax.rsqrt(variance + 1e-6)

    @pl.loop(1, n)
    def _(step):
        mod_copy(step, lax.rem(me - step + n, n)).wait_recv()

    @pl.loop(1, n)
    def _(step):
        gate_copy(step, me).start()

    modulation = jnp.sum(mods[...].astype(F32), axis=0)
    shift = modulation[0:1]
    scale = modulation[1:2]
    modulated = (norm_s[...] * (1.0 + scale) + shift).astype(BF16)
    loads[4].wait()
    spare = jnp.zeros((rows, send.shape[2] - 3 * head), BF16)
    part_heads = HEADS // 2

    def pair_copy(to, slot):
        return pltpu.make_async_remote_copy(
            src_ref=send.at[lax.rem(to, HEADS)],
            dst_ref=got.at[slot],
            send_sem=psend.at[to],
            recv_sem=precv.at[slot],
            device_id={"patch": to},
            device_id_type=MESH,
        )

    def make_half(half):
        low = half * part_heads * head
        start = low // 128 * 128
        stop = -(-(low + part_heads * head) // 128) * 128
        parts = [
            dot(modulated, qkv[:, i * width + start : i * width + stop]).astype(BF16)
            for i in range(3)
        ]
        for h in range(part_heads):
            cols = slice(low - start + h * head, low - start + (h + 1) * head)
            send[half * part_heads + h] = jnp.concatenate(
                [part[:, cols] for part in parts] + [spare], axis=1
            )

        @pl.loop(0, groups * part_heads)
        def _(j):
            turn = lax.rem(me + j, part_heads)
            to = (j // part_heads) * HEADS + half * part_heads + turn

            @pl.when(to != me)
            def _():
                pair_copy(to, me).start()

    @pl.when(my_head < part_heads)
    def _():
        make_half(1)
        make_half(0)

    @pl.when(my_head >= part_heads)
    def _():
        make_half(0)
        make_half(1)

    got[me] = send[my_head]
    tail = lax.broadcasted_iota(jnp.int32, (chunk, vbuf.shape[1] - head), 1)
    ones = jnp.where(tail == 0, 1.0, 0.0).astype(BF16)
    slot_ids = lax.broadcasted_iota(jnp.int32, (rows, 1), 0)
    lane_ids = lax.broadcasted_iota(jnp.int32, (rows, kbuf.shape[1]), 1)
    for g in range(groups):
        vbuf[g * chunk : (g + 1) * chunk, head:] = ones
    for b in range(n):
        bias = jnp.where(slot_ids < counts[b], 0.0, NEG)
        kbuf[b * rows : (b + 1) * rows, :] = jnp.where(lane_ids == head, bias, 0.0).astype(BF16)

    @pl.loop(1, n)
    def _(step):
        pair_copy(me, lax.rem(me - step + n, n)).wait_recv()

    for g in range(groups):
        block = got[g * HEADS : (g + 1) * HEADS].reshape(chunk, got.shape[2])
        kbuf[g * chunk : (g + 1) * chunk, :head] = block[:, head : 2 * head]
        vbuf[g * chunk : (g + 1) * chunk, :head] = block[:, 2 * head : 3 * head]


    def att_copy(j, slot, to):
        return pltpu.make_async_remote_copy(
            src_ref=att.at[j],
            dst_ref=back.at[slot],
            send_sem=asend.at[j],
            recv_sem=arecv.at[slot],
            device_id={"patch": group * HEADS + to},
            device_id_type=MESH,
        )

    pairs = HEADS // 4
    mine = my_head // pairs

    @pl.loop(0, HEADS // pairs)
    def _(step):
        base = lax.rem(mine // 2 + 1 + step // 2, 2) * 2 + lax.rem(mine + 1 + step, 2)
        base = base * pairs
        block = got[pl.ds(group * HEADS + base, pairs)].reshape(pairs * rows, got.shape[2])
        query = jnp.concatenate(
            [block[:, :head], jnp.ones((pairs * rows, 1), BF16)], axis=1
        )
        query = jnp.concatenate(
            [query, jnp.zeros((pairs * rows, kbuf.shape[1] - head - 1), BF16)], axis=1
        )
        top = weighted = None
        for g in range(groups):
            keys = kbuf[g * chunk : (g + 1) * chunk, :]
            scores = lax.dot_general(
                query, keys, (((1,), (1,)), ((), ())), preferred_element_type=F32
            )
            new_top = jnp.max(scores, axis=1, keepdims=True)
            if g:
                new_top = jnp.maximum(top, new_top)
            prob = jnp.exp2((scores - new_top) * inv_root).astype(BF16)
            mixed = dot(prob, vbuf[g * chunk : (g + 1) * chunk, :])
            if g:
                mixed = weighted * jnp.exp2((top - new_top) * inv_root) + mixed
            top, weighted = new_top, mixed
        total = weighted[:, head : head + 1]
        result = weighted / total
        for i in range(pairs):
            att[base + i] = fold(result[i * rows : (i + 1) * rows, :head]).astype(BF16)
        for i in range(pairs):

            @pl.when(base + i != my_head)
            def _():
                att_copy(base + i, my_head, base + i).start()

    back[my_head] = att[my_head]
    filler = jnp.zeros((rows, ow.shape[1] - head), F32)
    for load in ow_loads:
        load.wait()

    @pl.loop(1, n)
    def _(step):
        gate_copy(step, lax.rem(me - step + n, n)).wait_recv()

    gate_rows = jnp.sum(gates[...].astype(F32), axis=0)
    gate = jnp.concatenate([gate_rows[0:1], gate_rows[1:2, 2 * span - width :]], axis=1)

    @pl.loop(1, n)
    def _(step):
        mod_copy(step, me).wait_send()
        pair_copy(lax.rem(me + step, n), me).wait_send()
        gate_copy(step, me).wait_send()

    @pl.loop(1, HEADS)
    def _(step):
        other = lax.rem(my_head + step, HEADS)
        att_copy(other, other, other).wait_recv()

    attended = jnp.concatenate(
        [
            piece
            for h in range(HEADS)
            for piece in (unfold(back[h].astype(F32), rows, head - 64), filler)
        ],
        axis=1,
    ).astype(BF16)
    projected = dot(attended, ow[...].reshape(HEADS * ow.shape[1], width))
    valid = (lax.broadcasted_iota(jnp.int32, (rows, 1), 0) < counts[me]).astype(F32)
    out[...] = (xin_s[...] + gate * projected * valid).astype(BF16)

    @pl.loop(1, HEADS)
    def _(step):
        other = lax.rem(my_head + step, HEADS)
        att_copy(other, other, other).wait_send()


def tables(width, freq):
    quarter, half = width // 4, freq // 2
    omega = np.power(10000.0, -np.arange(quarter) / quarter)
    turn = math.pi / 2
    pos_tab = np.stack([np.tile(omega, 4), np.repeat([0.0, turn, 0.0, turn], quarter)])
    wave = np.exp(-math.log(10000.0) * np.arange(half) / half)
    time_tab = np.stack([np.tile(wave, 2), np.repeat([turn, 0.0], half)])
    return pos_tab.astype(np.float32), time_tab.astype(np.float32)


def per_device(
    tokens, positions, counts, timestep, time_in, time_out, ada_weight, qkv_weight, out_weight
):
    n = lax.axis_size("patch")
    rows, width = tokens.shape
    head = width // HEADS
    lane = 128
    head_pad = -(-head // lane) * lane
    pack = -(-3 * head // lane) * lane
    fold_back = rows // 2 + fold_group(rows, head - 64)
    pos_tab, time_tab = tables(width, time_in.shape[0])
    smem = pl.BlockSpec(memory_space=pltpu.SMEM)
    vmem = pl.BlockSpec(memory_space=pltpu.VMEM)
    hbm = pl.BlockSpec(memory_space=pl.ANY)
    result = pl.pallas_call(
        functools.partial(block_kernel, n, rows, width, head),
        out_shape=jax.ShapeDtypeStruct((rows, width), BF16),
        in_specs=[smem, smem, vmem, vmem, vmem] + [hbm] * 6,
        out_specs=vmem,
        scratch_shapes=[
            pltpu.VMEM(tokens.shape, BF16),
            pltpu.VMEM(time_in.shape, BF16),
            pltpu.VMEM(time_out.shape[::-1], BF16),
            pltpu.VMEM(ada_weight.shape, BF16),
            pltpu.VMEM(qkv_weight.shape, BF16),
            pltpu.VMEM((HEADS, head_pad, width), BF16),
            pltpu.VMEM((n, 2, width), BF16),
            pltpu.VMEM((n, 2, -(-width // 256) * 128), BF16),
            pltpu.VMEM((rows, width), F32),
            pltpu.VMEM((rows, width), F32),
            pltpu.VMEM((HEADS, rows, pack), BF16),
            pltpu.VMEM((n, rows, pack), BF16),
            pltpu.VMEM((n * rows, head_pad), BF16),
            pltpu.VMEM((n * rows, head_pad), BF16),
            pltpu.VMEM((HEADS, fold_back, lane), BF16),
            pltpu.VMEM((HEADS, fold_back, lane), BF16),
            pltpu.SemaphoreType.DMA((5,)),
            pltpu.SemaphoreType.DMA((HEADS,)),
            pltpu.SemaphoreType.DMA((n,)),
            pltpu.SemaphoreType.DMA((n,)),
            pltpu.SemaphoreType.DMA((n,)),
            pltpu.SemaphoreType.DMA((n,)),
            pltpu.SemaphoreType.DMA((n,)),
            pltpu.SemaphoreType.DMA((n,)),
            pltpu.SemaphoreType.DMA((HEADS,)),
            pltpu.SemaphoreType.DMA((HEADS,)),
        ],
        compiler_params=pltpu.CompilerParams(
            collective_id=0, has_side_effects=True, vmem_limit_bytes=60 * 2**20
        ),
    )(
        counts, timestep, positions, pos_tab, time_tab,
        tokens, time_in, time_out.T, ada_weight, qkv_weight, out_weight,
    )
    return result


def solution(mesh):
    placed = (
        P(("req", "patch"), None),
        P(None, ("req", "patch")),
        P("req"),
        P("req"),
        P(),
        P(None, "patch"),
        P("patch", None),
        P(),
        P(),
    )
    return jax.shard_map(
        per_device, mesh=mesh, in_specs=placed, out_specs=P(("req", "patch"), None), check_vma=False
    )
```

```python
import functools
import math

import jax
import jax.numpy as jnp
import numpy as np
from jax import lax
from jax.experimental import pallas as pl
from jax.experimental.pallas import tpu as pltpu
from jax.sharding import PartitionSpec as P

HEADS = 16
NEG = -1e30
F32 = jnp.float32
BF16 = jnp.bfloat16
MESH = pl.DeviceIdType.MESH


def silu(v):
    return v / (1.0 + jnp.exp(-v))


def dot(a, b):
    return jnp.dot(a, b, preferred_element_type=F32)


def one_row_dot(row, matrix):
    wide = jnp.broadcast_to(row, (16, row.shape[1])).astype(BF16)
    return dot(wide, matrix)[0:1]


def fold_group(rows, extra):
    group = 8
    while rows // group * extra > 128:
        group *= 2
    return group


def fold(block):
    rows, extra = block.shape[0], block.shape[1] - 64
    group = fold_group(rows, extra)
    half = rows // 2
    main = jnp.concatenate([block[:half, :64], block[half:, :64]], axis=1)
    pieces = [block[r : r + group, 64:] for r in range(0, rows, group)]
    spare = 128 - extra * len(pieces)
    rest = jnp.concatenate(pieces + [jnp.zeros((group, spare), F32)], axis=1)
    return jnp.concatenate([main, rest], axis=0)


def unfold(packed, rows, extra):
    half = rows // 2
    left = jnp.concatenate([packed[:half, :64], packed[:half, 64:]], axis=0)
    rest = packed[half:]
    count = rows // fold_group(rows, extra)
    right = jnp.concatenate([rest[:, r * extra : (r + 1) * extra] for r in range(count)], axis=0)
    return jnp.concatenate([left, right], axis=1)


def block_kernel(
    n, rows, width, head,
    counts, tstep, pos, pos_tab, time_tab,
    tok_h, tin_h, tout_h, ada_h, qkv_h, ow_h,
    out,
    tok, tin, tout, ada, qkv, ow, mods, gates, xin_s, norm_s, send, got, kbuf, vbuf, att, back,
    done, osem, lsem, wsem, msend, mrecv, gsend, grecv, psend, precv, asend, arecv,
):
    me = lax.axis_index("patch")
    my_head = lax.rem(me, HEADS)
    group = me // HEADS
    chunk = HEADS * rows
    groups = n // HEADS
    inv_root = math.log2(math.e) / math.sqrt(head)

    barrier = pltpu.get_barrier_semaphore()

    @pl.loop(1, n)
    def _(step):
        pl.semaphore_signal(
            barrier, inc=1, device_id={"patch": lax.rem(me + step, n)}, device_id_type=MESH
        )

    loads = [
        pltpu.make_async_copy(src, dst, lsem.at[i])
        for i, (src, dst) in enumerate(
            [(tin_h, tin), (tout_h, tout), (ada_h, ada), (tok_h, tok), (qkv_h, qkv)]
        )
    ]
    for load in loads[:3]:
        load.start()

    angles = tstep[0].astype(F32) * time_tab[0:1, :] + time_tab[1:2, :]
    features = jnp.sin(angles).astype(BF16)
    loads[0].wait()
    hidden = silu(one_row_dot(features, tin[...])).astype(BF16)
    loads[1].wait()
    wide = jnp.broadcast_to(hidden, (16, width))
    cond = lax.dot_general(wide, tout[...], (((1,), (1,)), ((), ())), preferred_element_type=F32)
    activated = silu(cond[0:1]).astype(BF16)
    loads[2].wait()
    partial = one_row_dot(activated, ada[...])
    mods[me] = jnp.concatenate(
        [partial[:, :width], partial[:, width : 2 * width]], axis=0
    ).astype(BF16)
    span = gates.shape[2]
    gates[me] = jnp.concatenate(
        [partial[:, 2 * width : 2 * width + span], partial[:, 3 * width - span :]], axis=0
    ).astype(BF16)
    for load in loads[3:]:
        load.start()

    pl.semaphore_wait(barrier, n - 1)

    def mod_copy(step, slot):
        return pltpu.make_async_remote_copy(
            src_ref=mods.at[slot],
            dst_ref=mods.at[slot],
            send_sem=msend.at[step],
            recv_sem=mrecv.at[slot],
            device_id={"patch": lax.rem(me + step, n)},
            device_id_type=MESH,
        )

    def gate_copy(step, slot):
        return pltpu.make_async_remote_copy(
            src_ref=gates.at[slot],
            dst_ref=gates.at[slot],
            send_sem=gsend.at[step],
            recv_sem=grecv.at[slot],
            device_id={"patch": lax.rem(me + step, n)},
            device_id_type=MESH,
        )

    @pl.loop(1, n)
    def _(step):
        mod_copy(step, me).start()

    ow[:, head:, :] = jnp.zeros((HEADS, ow.shape[1] - head, width), BF16)
    ow_loads = [
        pltpu.make_async_copy(
            ow_h.at[pl.ds(h * head, head), :], ow.at[h, pl.ds(0, head), :], wsem.at[h]
        )
        for h in range(HEADS)
    ]
    for load in ow_loads:
        load.start()

    ids = lax.broadcasted_iota(jnp.int32, (rows, rows), 0)
    eye = ids == lax.broadcasted_iota(jnp.int32, (rows, rows), 1)
    posf = pos[...].astype(F32)
    row_col = jnp.sum(jnp.where(eye, posf[0:1, :], 0.0), axis=1, keepdims=True)
    col_col = jnp.sum(jnp.where(eye, posf[1:2, :], 0.0), axis=1, keepdims=True)
    lanes = lax.broadcasted_iota(jnp.int32, (1, width), 1)
    first = lanes < width // 2
    place = jnp.where(first, row_col, col_col)
    embed = jnp.sin(place * pos_tab[0:1, :] + pos_tab[1:2, :])
    loads[3].wait()
    x_in = tok[...].astype(F32) + embed
    xin_s[...] = x_in
    centered = x_in - jnp.mean(x_in, axis=1, keepdims=True)
    variance = jnp.mean(centered * centered, axis=1, keepdims=True)
    norm_s[...] = centered * lax.rsqrt(variance + 1e-6)

    @pl.loop(1, n)
    def _(step):
        mod_copy(step, lax.rem(me - step + n, n)).wait_recv()

    @pl.loop(1, n)
    def _(step):
        gate_copy(step, me).start()

    modulation = jnp.sum(mods[...].astype(F32), axis=0)
    shift = modulation[0:1]
    scale = modulation[1:2]
    modulated = (norm_s[...] * (1.0 + scale) + shift).astype(BF16)
    loads[4].wait()
    spare = jnp.zeros((rows, send.shape[2] - 3 * head), BF16)
    part_heads = HEADS // 2

    def pair_copy(to, slot):
        return pltpu.make_async_remote_copy(
            src_ref=send.at[lax.rem(to, HEADS)],
            dst_ref=got.at[slot],
            send_sem=psend.at[to],
            recv_sem=precv.at[slot],
            device_id={"patch": to},
            device_id_type=MESH,
        )

    def make_half(half):
        low = half * part_heads * head
        start = low // 128 * 128
        stop = -(-(low + part_heads * head) // 128) * 128
        parts = [
            dot(modulated, qkv[:, i * width + start : i * width + stop]).astype(BF16)
            for i in range(3)
        ]
        for h in range(part_heads):
            cols = slice(low - start + h * head, low - start + (h + 1) * head)
            send[half * part_heads + h] = jnp.concatenate(
                [part[:, cols] for part in parts] + [spare], axis=1
            )

        @pl.loop(0, groups * part_heads)
        def _(j):
            turn = lax.rem(me + j, part_heads)
            to = (j // part_heads) * HEADS + half * part_heads + turn

            @pl.when(to != me)
            def _():
                pair_copy(to, me).start()

    @pl.when(my_head < part_heads)
    def _():
        make_half(1)
        make_half(0)

    @pl.when(my_head >= part_heads)
    def _():
        make_half(0)
        make_half(1)

    got[me] = send[my_head]
    tail = lax.broadcasted_iota(jnp.int32, (chunk, vbuf.shape[1] - head), 1)
    ones = jnp.where(tail == 0, 1.0, 0.0).astype(BF16)
    slot_ids = lax.broadcasted_iota(jnp.int32, (rows, 1), 0)
    lane_ids = lax.broadcasted_iota(jnp.int32, (rows, kbuf.shape[1]), 1)
    for g in range(groups):
        vbuf[g * chunk : (g + 1) * chunk, head:] = ones
    for b in range(n):
        bias = jnp.where(slot_ids < counts[b], 0.0, NEG)
        kbuf[b * rows : (b + 1) * rows, :] = jnp.where(lane_ids == head, bias, 0.0).astype(BF16)

    @pl.loop(1, n)
    def _(step):
        pair_copy(me, lax.rem(me - step + n, n)).wait_recv()

    for g in range(groups):
        block = got[g * HEADS : (g + 1) * HEADS].reshape(chunk, got.shape[2])
        kbuf[g * chunk : (g + 1) * chunk, :head] = block[:, head : 2 * head]
        vbuf[g * chunk : (g + 1) * chunk, :head] = block[:, 2 * head : 3 * head]


    def att_copy(j, slot, to):
        return pltpu.make_async_remote_copy(
            src_ref=att.at[j],
            dst_ref=back.at[slot],
            send_sem=asend.at[j],
            recv_sem=arecv.at[slot],
            device_id={"patch": group * HEADS + to},
            device_id_type=MESH,
        )

    pairs = HEADS // 4
    mine = my_head // pairs

    @pl.loop(0, HEADS // pairs)
    def _(step):
        base = lax.rem(mine // 2 + 1 + step // 2, 2) * 2 + lax.rem(mine + 1 + step, 2)
        base = base * pairs
        block = got[pl.ds(group * HEADS + base, pairs)].reshape(pairs * rows, got.shape[2])
        query = jnp.concatenate(
            [block[:, :head], jnp.ones((pairs * rows, 1), BF16)], axis=1
        )
        query = jnp.concatenate(
            [query, jnp.zeros((pairs * rows, kbuf.shape[1] - head - 1), BF16)], axis=1
        )
        top = weighted = None
        for g in range(groups):
            keys = kbuf[g * chunk : (g + 1) * chunk, :]
            scores = lax.dot_general(
                query, keys, (((1,), (1,)), ((), ())), preferred_element_type=F32
            )
            new_top = jnp.max(scores, axis=1, keepdims=True)
            if g:
                new_top = jnp.maximum(top, new_top)
            prob = jnp.exp2((scores - new_top) * inv_root).astype(BF16)
            mixed = dot(prob, vbuf[g * chunk : (g + 1) * chunk, :])
            if g:
                mixed = weighted * jnp.exp2((top - new_top) * inv_root) + mixed
            top, weighted = new_top, mixed
        total = weighted[:, head : head + 1]
        result = weighted / total
        for i in range(pairs):
            att[base + i] = fold(result[i * rows : (i + 1) * rows, :head]).astype(BF16)
        for i in range(pairs):

            @pl.when(base + i != my_head)
            def _():
                att_copy(base + i, my_head, base + i).start()

    back[my_head] = att[my_head]
    filler = jnp.zeros((rows, ow.shape[1] - head), F32)
    for load in ow_loads:
        load.wait()

    @pl.loop(1, n)
    def _(step):
        gate_copy(step, lax.rem(me - step + n, n)).wait_recv()

    gate_rows = jnp.sum(gates[...].astype(F32), axis=0)
    gate = jnp.concatenate([gate_rows[0:1], gate_rows[1:2, 2 * span - width :]], axis=1)

    @pl.loop(1, n)
    def _(step):
        mod_copy(step, me).wait_send()
        pair_copy(lax.rem(me + step, n), me).wait_send()
        gate_copy(step, me).wait_send()

    @pl.loop(1, HEADS)
    def _(step):
        other = lax.rem(my_head + step, HEADS)
        att_copy(other, other, other).wait_recv()

    attended = jnp.concatenate(
        [
            piece
            for h in range(HEADS)
            for piece in (unfold(back[h].astype(F32), rows, head - 64), filler)
        ],
        axis=1,
    ).astype(BF16)
    weight = ow[...].reshape(HEADS * ow.shape[1], width)
    valid = (lax.broadcasted_iota(jnp.int32, (rows, 1), 0) < counts[me]).astype(F32)
    cut = width // 256 * 128
    stores = []
    for i, cols in enumerate([slice(0, cut), slice(cut, width)]):
        projected = dot(attended, weight[:, cols])
        done[:, cols] = (xin_s[:, cols] + gate[:, cols] * projected * valid).astype(BF16)
        stores.append(pltpu.make_async_copy(done.at[:, cols], out.at[:, cols], osem.at[i]))
        stores[-1].start()

    @pl.loop(1, HEADS)
    def _(step):
        other = lax.rem(my_head + step, HEADS)
        att_copy(other, other, other).wait_send()

    for store in stores:
        store.wait()


def tables(width, freq):
    quarter, half = width // 4, freq // 2
    omega = np.power(10000.0, -np.arange(quarter) / quarter)
    turn = math.pi / 2
    pos_tab = np.stack([np.tile(omega, 4), np.repeat([0.0, turn, 0.0, turn], quarter)])
    wave = np.exp(-math.log(10000.0) * np.arange(half) / half)
    time_tab = np.stack([np.tile(wave, 2), np.repeat([turn, 0.0], half)])
    return pos_tab.astype(np.float32), time_tab.astype(np.float32)


def per_device(
    tokens, positions, counts, timestep, time_in, time_out, ada_weight, qkv_weight, out_weight
):
    n = lax.axis_size("patch")
    rows, width = tokens.shape
    head = width // HEADS
    lane = 128
    head_pad = -(-head // lane) * lane
    pack = -(-3 * head // lane) * lane
    fold_back = rows // 2 + fold_group(rows, head - 64)
    pos_tab, time_tab = tables(width, time_in.shape[0])
    smem = pl.BlockSpec(memory_space=pltpu.SMEM)
    vmem = pl.BlockSpec(memory_space=pltpu.VMEM)
    hbm = pl.BlockSpec(memory_space=pl.ANY)
    result = pl.pallas_call(
        functools.partial(block_kernel, n, rows, width, head),
        out_shape=jax.ShapeDtypeStruct((rows, width), BF16),
        in_specs=[smem, smem, vmem, vmem, vmem] + [hbm] * 6,
        out_specs=hbm,
        scratch_shapes=[
            pltpu.VMEM(tokens.shape, BF16),
            pltpu.VMEM(time_in.shape, BF16),
            pltpu.VMEM(time_out.shape[::-1], BF16),
            pltpu.VMEM(ada_weight.shape, BF16),
            pltpu.VMEM(qkv_weight.shape, BF16),
            pltpu.VMEM((HEADS, head_pad, width), BF16),
            pltpu.VMEM((n, 2, width), BF16),
            pltpu.VMEM((n, 2, -(-width // 256) * 128), BF16),
            pltpu.VMEM((rows, width), F32),
            pltpu.VMEM((rows, width), F32),
            pltpu.VMEM((HEADS, rows, pack), BF16),
            pltpu.VMEM((n, rows, pack), BF16),
            pltpu.VMEM((n * rows, head_pad), BF16),
            pltpu.VMEM((n * rows, head_pad), BF16),
            pltpu.VMEM((HEADS, fold_back, lane), BF16),
            pltpu.VMEM((HEADS, fold_back, lane), BF16),
            pltpu.VMEM((rows, width), BF16),
            pltpu.SemaphoreType.DMA((2,)),
            pltpu.SemaphoreType.DMA((5,)),
            pltpu.SemaphoreType.DMA((HEADS,)),
            pltpu.SemaphoreType.DMA((n,)),
            pltpu.SemaphoreType.DMA((n,)),
            pltpu.SemaphoreType.DMA((n,)),
            pltpu.SemaphoreType.DMA((n,)),
            pltpu.SemaphoreType.DMA((n,)),
            pltpu.SemaphoreType.DMA((n,)),
            pltpu.SemaphoreType.DMA((HEADS,)),
            pltpu.SemaphoreType.DMA((HEADS,)),
        ],
        compiler_params=pltpu.CompilerParams(
            collective_id=0, has_side_effects=True, vmem_limit_bytes=60 * 2**20
        ),
    )(
        counts, timestep, positions, pos_tab, time_tab,
        tokens, time_in, time_out.T, ada_weight, qkv_weight, out_weight,
    )
    return result


def solution(mesh):
    placed = (
        P(("req", "patch"), None),
        P(None, ("req", "patch")),
        P("req"),
        P("req"),
        P(),
        P(None, "patch"),
        P("patch", None),
        P(),
        P(),
    )
    return jax.shard_map(
        per_device, mesh=mesh, in_specs=placed, out_specs=P(("req", "patch"), None), check_vma=False
    )
```
